32 devices in a mesh: grp: 4 (over z), row: 4 (over x, core), col: 2 (over y).
Axes of the slice: x: 2, y: 2, z: 4, core: 2. Of those that a mesh axis runs over, the one named last changes fastest.
Arguments:
- acts: bfloat16 [768, 8192], P('grp', 'col'), may hold values from -6 to 6
- grads: bfloat16 [768, 28672], P('grp', ('row', 'col')), may hold values from -6 to 6
- basis_in: bfloat16 [8192, 4096], P('col', 'row'), may hold values from -0.0625 to 0.0625
- basis_out: bfloat16 [4, 7168, 14336], P('row', 'grp', 'col'), may hold values from -0.03125 to 0.03125
- lengths: int32 [4, 2], P('grp'), may hold values from 1 to 96, 144 in all within a row
Outputs:
- eigenvalues: float32 [14336, 4096], P('col', 'row')
The draws below stay inside these ranges and needn't reach their ends.
Inputs may be any that keep to these rules, and one draw needn't show every extreme that they name: The 2 lengths of each index of grp sum to exactly 144, and none exceeds 96.
All inputs are finite; a program needn't handle non-finite values.
Results may differ from the reference program's by a relative error of at most 0.006.
Values may be sent and summed in bfloat16 or wider, within the bound.
A program may use at most 256 MiB of HBM per device.

```python
import math
import jax
import jax.numpy as jnp
import numpy as np
from jax import lax

FI = 8192
FO = 28672
IW = 4096
GW = 14336
LEN = 96
SEQS = 2
VALID = 144
TOKENS = 768
N_GRP = 4
N_ROW = 4


def levels(stream_key, dims, shards, least, largest):
    factor_of = 1.0
    for position, blocks in shards:
        steps = jax.random.uniform(jax.random.fold_in(jax.random.fold_in(stream_key, 6), position), (blocks,), jnp.float32, least / len(shards), largest / len(shards))
        factor_of = factor_of * jnp.repeat(jnp.exp(steps), dims[position] // blocks).reshape((-1,) + (1,) * (len(dims) - 1 - position))
    return factor_of


def profile(count, total, reach, skew):
    loads = [(1 << 20) // math.isqrt(standing ** skew) + 1 for standing in range(2, count + 1)]
    rest, counts = total - reach - (count - 1), [1] * (count - 1)
    while rest > 0:
        candidates = [i for i in range(count - 1) if counts[i] < reach]
        mass, remaining = sum([loads[i] for i in candidates]), rest
        for i in candidates:
            extra = min(reach - counts[i], max(1, remaining * loads[i] // mass), rest)
            counts[i] = counts[i] + extra
            rest = rest - extra
    return np.array([reach] + counts)


def ragged(own_key, count, total, reach, lean):
    if count == 2:
        one = jax.random.randint(own_key, (), max(1, total - reach), min(reach, total - 1) + 1)
        return jnp.stack([one, total - one])
    sizes = jnp.asarray(profile(count, total, reach, lean), jnp.int32)
    couples = (count - 1) // 2
    source_of, sink = sizes[1:1 + 2 * couples:2], sizes[2:2 + 2 * couples:2]
    slack = jnp.minimum(source_of - 1, reach - sink)
    shifted = jax.random.randint(jax.random.fold_in(own_key, 1), (couples,), 0, 1 << 20) % (slack + 1)
    sizes = sizes.at[1:1 + 2 * couples:2].set(source_of - shifted).at[2:2 + 2 * couples:2].set(sink + shifted)
    return sizes[jax.random.permutation(jax.random.fold_in(own_key, 2), count)]


def bell_draw(key, dims, spread, most, shards=(), kind=jnp.bfloat16):
    entries = jax.random.normal(key, dims, jnp.float32) * spread
    if len(shards) > 0:
        entries = levels(key, dims, shards, -0.22, 0.18) * entries
    return jnp.clip(entries, min=-most, max=most).astype(kind)


def setup_inputs(seed: int = 0) -> dict:
    key_list = jax.random.split(jax.random.key(seed), 6)
    return {
        "acts": bell_draw(key_list[0], (TOKENS, FI), 1.0, 6.0, ((0, 4), (1, 2))),
        "grads": bell_draw(key_list[1], (TOKENS, FO), 1.0, 6.0, ((0, 4), (1, 8))),
        "basis_in": bell_draw(key_list[2], (FI, IW), FI ** -0.5, 0.0625, ((0, 2), (1, 4))),
        "basis_out": bell_draw(key_list[3], (N_ROW, FO // N_ROW, GW), FO ** -0.5, 0.03125, ((0, 4), (1, 4), (2, 2))),
        "lengths": jax.vmap(lambda own: ragged(own, SEQS, VALID, LEN, 2))(jax.random.split(key_list[4], N_GRP)).reshape((N_GRP, SEQS)).astype(jnp.int32),
    }


def reference(acts, grads, basis_in, basis_out, lengths):
    proj_in = jnp.dot(acts, basis_in, preferred_element_type=jnp.float32).astype(jnp.bfloat16)
    whole_basis = basis_out.reshape(FO, GW)
    proj_out = jnp.dot(grads, whole_basis, preferred_element_type=jnp.float32).astype(jnp.bfloat16)
    count = N_GRP * SEQS
    slots = jnp.arange(LEN).astype(jnp.int32)
    valid = (slots[None, None, :] < lengths[:, :, None]).reshape(count, LEN).astype(proj_out.dtype)

    def step(total, item):
        grad_seq, act_seq, keep = item
        chosen = grad_seq * keep[:, None]
        block = jnp.dot(chosen.T, act_seq, preferred_element_type=jnp.float32)
        return total + block * block, None

    total, unused = lax.scan(step, jnp.zeros((GW, IW), jnp.float32),
                             (proj_out.reshape(count, LEN, GW), proj_in.reshape(count, LEN, IW), valid))
    return total / (count * LEN)
```

```python
import functools

import jax
import jax.numpy as jnp
from jax import lax
from jax.experimental import pallas as pl
from jax.experimental.pallas import tpu as pltpu
from jax.sharding import PartitionSpec as P

LEN = 96
VALID = 144
LANES = 128


def squares_kernel(groups, count, scale, left_ref, right_ref, out_ref):
    valid = left_ref.shape[0] // groups
    wide = out_ref.shape[1]
    chunk = 256 if wide % 256 == 0 else wide
    for begin in range(0, wide, chunk):
        total = None
        for group in range(groups):
            left = left_ref[pl.ds(group * valid, valid), :]
            for seq in range(count):
                right = right_ref[group * count + seq, :, pl.ds(begin, chunk)]
                block = lax.dot_general(
                    left, right, (((0,), (0,)), ((), ())), preferred_element_type=jnp.float32
                )
                total = block * block if total is None else total + block * block
        out_ref[:, pl.ds(begin, chunk)] = total * scale


def sum_of_squares(left, right, groups, count, scale):
    rows, columns = left.shape[1], right.shape[2]
    tile = rows
    for size in (512, 384, 256, 128):
        if rows % size == 0:
            tile = size
            break
    return pl.pallas_call(
        functools.partial(squares_kernel, groups, count, scale),
        grid=(rows // tile,),
        out_shape=jax.ShapeDtypeStruct((rows, columns), jnp.float32),
        in_specs=[
            pl.BlockSpec((left.shape[0], tile), lambda i: (0, i)),
            pl.BlockSpec(right.shape, lambda i: (0, 0, 0)),
        ],
        out_specs=pl.BlockSpec((tile, columns), lambda i: (i, 0)),
        cost_estimate=pl.CostEstimate(
            flops=2 * count * left.shape[0] * rows * columns,
            bytes_accessed=4 * rows * columns,
            transcendentals=0,
        ),
        compiler_params=pltpu.CompilerParams(vmem_limit_bytes=48 * 1024 * 1024),
    )(left, right)


def packing(seq_lens):
    count = seq_lens.shape[0]
    ends = jnp.cumsum(seq_lens)
    starts = ends - seq_lens
    slot_ids = jnp.arange(VALID, dtype=jnp.int32)
    segment = jnp.sum((slot_ids[:, None] >= ends[None, :]).astype(jnp.int32), axis=1)
    member = segment[:, None] == jnp.arange(count, dtype=jnp.int32)[None, :]
    offset = jnp.sum(jnp.where(member, starts[None, :], 0), axis=1)
    return segment * LEN + slot_ids - offset, segment


def per_device(acts, grads, basis_in, basis_out, lengths):
    seq_lens = lengths[0]
    count = seq_lens.shape[0]
    groups = lax.axis_size("grp")
    source, segment = packing(seq_lens)

    packed = jnp.take(grads, source, axis=0)
    gathered = lax.all_gather(packed, "col", axis=1, tiled=True)
    mine = lax.all_to_all(gathered, "grp", split_axis=1, concat_axis=0, tiled=True)
    partial_out = jnp.dot(mine, basis_out[0], preferred_element_type=jnp.float32)
    partial_out = partial_out.astype(jnp.bfloat16)

    partial_in = jnp.dot(
        jnp.take(acts, source, axis=0), basis_in, preferred_element_type=jnp.float32
    )
    proj_in = lax.psum(partial_in, "col").astype(jnp.bfloat16)
    tag = jnp.broadcast_to(segment[:, None].astype(jnp.bfloat16), (VALID, LANES))
    tagged = jnp.concatenate([proj_in, tag], axis=1)
    tagged = lax.all_gather(tagged, "grp", axis=0, tiled=False)
    every_in = tagged[:, :, : proj_in.shape[1]]
    member = tagged[:, None, :, proj_in.shape[1]] == jnp.arange(count, dtype=jnp.bfloat16)[None, :, None]
    masked = jnp.where(member[..., None], every_in[:, None], 0)
    masked = masked.reshape(groups * count, VALID, proj_in.shape[1])

    part = lax.psum_scatter(partial_out, "row", scatter_dimension=0, tiled=True)
    part = lax.psum_scatter(part, "grp", scatter_dimension=1, tiled=True)
    proj_out = lax.all_gather(part, "grp", axis=1, tiled=True)
    proj_out = lax.all_gather(proj_out, "row", axis=0, tiled=True)
    return sum_of_squares(proj_out, masked, groups, count, 1.0 / (groups * count * LEN))


def solution(mesh):
    in_specs = (
        P("grp", "col"),
        P("grp", ("row", "col")),
        P("col", "row"),
        P("row", "grp", "col"),
        P("grp", None),
    )
    out_specs = P("col", "row")
    return jax.shard_map(
        per_device, mesh=mesh, in_specs=in_specs, out_specs=out_specs, check_vma=False
    )
```
